1024 devices in a mesh: pipe: 4 (over y_hi, core), expert: 64 (over z, x), tensor: 4 (over y_lo).
Axes of the slice: x: 8, y: 8 (y_hi: 2, y_lo: 4; y = y_hi * 4 + y_lo), z: 8, core: 2. Of those that a mesh axis runs over, the one named last changes fastest.
Arguments:
- stream: bfloat16 [2, 4, 1024, 7168], P(None, 'pipe', 'expert', 'tensor'), may hold values from -6 to 6
- expert_ids: int32 [2, 4, 1024, 8], P(None, 'pipe', 'expert'), may hold values from 0 to 63, all different within a row; in each aligned block of 16 rows (0 to 15, 16 to 31, ..., all dimensions but the last counted through in order) at most 3 rows name the same one
- norm_gain: float32 [4, 7168], P('pipe', 'tensor'), may hold values from 0.1 to 1.9
- router: float32 [4, 7168, 64], P('pipe', 'tensor'), may hold values from -0.0625 to 0.0625
- w_up: bfloat16 [64, 7168, 1024], P('expert', 'tensor'), may hold values from -0.0625 to 0.0625
- w_down: bfloat16 [64, 1024, 7168], P('expert', None, 'tensor'), may hold values from -0.1875 to 0.1875
Outputs:
- result: bfloat16 [2, 4, 1024, 7168], P(None, 'pipe', 'expert', 'tensor')
The draws below stay inside these ranges and needn't reach their ends.
Inputs may be any that keep to these rules, and one draw needn't show every extreme that they name: `expert_ids`: each token names 8 different experts. Among the 16 tokens of one direction held by one index of the expert axis at one section, at most 3 name any one expert, and in every draw some expert is named by exactly 3 of them.
All inputs are finite; a program needn't handle non-finite values.
Results may differ from the reference program's by a relative error of at most 0.0065.
Values may be sent and summed in bfloat16 or wider, within the bound.
A program may use at most 32 MiB of HBM per device.

```python
import math
import jax
import jax.numpy as jnp
import numpy as np
from jax import lax

D = 7168
FF = 1024
TOK_DEV = 16
PIPE = 4
EXPERTS = 64
TOP = 8
TOKENS = 1024
CAP = 3
N_EXPERT = 64


def shard_levels(stream_key, extent, split, smallest, top_value):
    factor_of, own = 1.0, jax.random.fold_in(stream_key, 6)
    for position, blocks in split:
        draws = jnp.exp(jax.random.uniform(jax.random.fold_in(own, position), (blocks,), jnp.float32, smallest / len(split), top_value / len(split)))
        factor_of = factor_of * jnp.repeat(draws, extent[position] // blocks).reshape([-1 if axis == position else 1 for axis in range(len(extent))])
    return factor_of


def shared_out(own_key, own, number, rows, count, top, bound, skew):
    order = jax.random.permutation(own_key, count)
    heavy_load, usual = shares(count, rows * top, bound, skew, True), shares(count, rows * top, bound, skew, False)
    places = jnp.arange(count)

    def named(lengths, rotation):
        used = int((lengths > 0).sum())
        fixed = max(1, used // 4)
        moved = fixed + (places - fixed + rotation * (used - fixed)) % max(1, count - fixed)
        return jnp.zeros((count,), jnp.int32).at[order[jnp.where(places < fixed, places, moved)]].set(jnp.asarray(lengths, jnp.int32))

    lengths = jnp.where(number % 4 == 0, named(heavy_load, number // 4), named(usual, number - number // 4 - 1))
    mixed = jax.random.permutation(jax.random.fold_in(own, 3), count)
    source_of, sink = mixed[0:count // 2 * 2:2], mixed[1:count // 2 * 2:2]
    slack = jnp.minimum(lengths[source_of] - 1, bound - lengths[sink]) // 2
    slack = jnp.where((source_of == order[0]) | (sink == order[0]) | (lengths[sink] == 0), 0, jnp.maximum(slack, 0))
    moved = jax.random.randint(jax.random.fold_in(own, 4), (count // 2,), 0, 1 << 20) % (slack + 1)
    lengths = lengths.at[source_of].add(-moved).at[sink].add(moved)
    items = jnp.searchsorted(jnp.cumsum(lengths), jnp.arange(rows * top), side="right").astype(jnp.int32)
    listing = items.reshape(top, rows).T
    listing = listing[jax.random.permutation(jax.random.fold_in(own, 1), rows)]
    rotation = jax.random.randint(jax.random.fold_in(own, 2), (rows, 1), 0, top)
    return jnp.take_along_axis(listing, (jnp.arange(top)[None, :] + rotation) % top, axis=1)


def shares(count, total, limit, lean, full):
    portions = [(1 << 20) // math.isqrt(grade ** lean) + 1 for grade in range(1, count + 1)]
    largest = limit if full else min(limit, max(-(-total // count), total * portions[0] // sum(portions)))
    least = 1 if total - largest >= count - 1 else 0
    counts, rest = [largest] + [least] * (count - 1), total - largest - least * (count - 1)
    while rest > 0:
        free = [i for i in range(1, count) if counts[i] < largest] or [i for i in range(1, count) if counts[i] < limit]
        mass, budget = sum([portions[i] for i in free]), rest
        for i in free:
            addition = min(limit - counts[i], max(1, budget * portions[i] // mass), rest)
            counts[i] = counts[i] + addition
            rest = rest - addition
    return np.array(counts)


def scatter_about(own_key, extent, scale, most, split=(), held_as=jnp.bfloat16):
    loudness = shard_levels(own_key, extent, split, -0.22, 0.18) if split else 1.0
    values = jax.random.normal(own_key, extent, jnp.float32) * scale * loudness
    return jnp.minimum(jnp.maximum(values, -most), most).astype(held_as)


def setup_inputs(seed: int = 0) -> dict:
    splits = jax.random.split(jax.random.key(seed), 7)
    stream = scatter_about(splits[0], (2, PIPE, TOKENS, D), 1.0, 6.0, ((1, 4), (2, 64), (3, 4)))
    expert_ids_keys = jax.random.split(jax.random.fold_in(splits[1], 1), 2 * PIPE * TOKENS // TOK_DEV)
    expert_ids_turns = jax.random.permutation(jax.random.fold_in(splits[1], 3), 2 * PIPE * TOKENS // TOK_DEV)
    expert_ids = jax.vmap(lambda own, number: shared_out(jax.random.fold_in(splits[1], 2), own, number, TOK_DEV, EXPERTS, TOP, CAP, 2))(expert_ids_keys, expert_ids_turns).reshape((2, PIPE, TOKENS, TOP))
    norm_gain = jnp.clip(1.0 + 0.18 * jax.random.normal(splits[2], (PIPE, D), jnp.float32), 0.1, 1.9)
    router = scatter_about(splits[3], (PIPE, D, EXPERTS), D ** -0.5, 0.0625, ((0, 4), (1, 4)), jnp.float32)
    w_up = scatter_about(splits[4], (EXPERTS, D, FF), D ** -0.5, 0.0625, ((0, 64), (1, 4)))
    w_down = scatter_about(splits[5], (EXPERTS, FF, D), FF ** -0.5, 0.1875, ((0, 64), (2, 4)))
    return dict(stream=stream, expert_ids=expert_ids, norm_gain=norm_gain, router=router, w_up=w_up, w_down=w_down)


norm_eps = 1e-06
route_scale = 2.5

def reference(stream, expert_ids, norm_gain, router, w_up, w_down):
    ahead = jnp.roll(stream[0], 1, axis=0)
    behind = jnp.roll(stream[1], -1, axis=0)
    arrived = jnp.stack([ahead, behind]).astype(jnp.float32)
    inverse = lax.rsqrt(lax.optimization_barrier(jnp.mean(arrived * arrived, axis=-1)) + norm_eps)
    normed = arrived * norm_gain[None, :, None, :] * inverse[..., None]
    logits = jnp.einsum('dptc,pce->dpte', normed, router, precision=lax.Precision.HIGHEST)
    picked = jnp.take_along_axis(logits, expert_ids, axis=-1)
    scores = jax.nn.sigmoid(picked)
    gates = route_scale * scores / lax.optimization_barrier(jnp.sum(scores, axis=-1, keepdims=True))
    hidden = normed.astype(jnp.bfloat16)
    groups = expert_ids.reshape(2, PIPE, N_EXPERT, TOK_DEV * TOP)
    onehot = (groups[..., None] == jnp.arange(EXPERTS, dtype=jnp.int32)).astype(jnp.int32)
    earlier = jnp.cumsum(onehot, axis=3) - onehot
    within = lax.optimization_barrier(jnp.sum(earlier * onehot, axis=-1))
    heading = lax.broadcasted_iota(jnp.int32, groups.shape, 0)
    section = lax.broadcasted_iota(jnp.int32, groups.shape, 1)
    member = lax.broadcasted_iota(jnp.int32, groups.shape, 2)
    entry = lax.broadcasted_iota(jnp.int32, groups.shape, 3)
    place = ((section * N_EXPERT + member) * 2 + heading) * CAP + within
    anchor = ((heading * PIPE + section) * N_EXPERT + member) * TOK_DEV + entry // TOP
    length = PIPE * N_EXPERT * 2 * CAP
    owner = jnp.full((EXPERTS, length), 2 * PIPE * TOKENS, jnp.int32).at[groups, place].set(anchor)
    width = hidden.shape[-1]
    table = jnp.concatenate([hidden.reshape(-1, width), jnp.zeros((1, width), jnp.bfloat16)], axis=0)

    def expert_rows(pieces):
        owned, upper, lower = pieces
        inner = jnp.dot(table[owned], upper, preferred_element_type=jnp.float32)
        active = jax.nn.silu(inner).astype(jnp.bfloat16)
        return jnp.dot(active, lower, preferred_element_type=jnp.float32).astype(jnp.bfloat16)
    produced = lax.map(expert_rows, (owner, w_up, w_down))

    def combine(pieces):
        chosen, spots, weights = pieces
        rows = produced[chosen, spots].astype(jnp.float32)
        rows = rows.reshape(N_EXPERT * TOK_DEV, TOP, width)
        return jnp.einsum('tk,tkc->tc', weights, rows)
    mixed = lax.map(combine, (groups.reshape(2 * PIPE, N_EXPERT, TOK_DEV * TOP), place.reshape(2 * PIPE, N_EXPERT, TOK_DEV * TOP), gates.reshape(2 * PIPE, TOKENS, TOP)))
    result = arrived + mixed.reshape(arrived.shape)
    return result.astype(jnp.bfloat16)
```

```python
import functools

import jax
import jax.numpy as jnp
from jax import lax
from jax.experimental import pallas as pl
from jax.experimental.pallas import tpu as pltpu
from jax.sharding import PartitionSpec as P

norm_eps = 1e-06
route_scale = 2.5
MESH = pl.DeviceIdType.MESH
BF = jnp.bfloat16
F32 = jnp.float32
LANES = 128


def over(v, n, limit):
    m = -(-65536 // n)
    assert all((i * m) >> 16 == i // n for i in range(limit))
    return (v * m) >> 16


def split3(v):
    hi = v.astype(BF)
    rest = v - hi.astype(F32)
    mid = rest.astype(BF)
    low = (rest - mid.astype(F32)).astype(BF)
    return hi, mid, low


def nt_dot(a, b):
    return lax.dot_general(a, b, (((1,), (1,)), ((), ())), preferred_element_type=F32)


def mm(a, b):
    return jnp.dot(a, b, preferred_element_type=F32)


def layer(
    cfg, stream, ids, gain, router, w_up, w_down, out,
    up, down, rparts, arr, blocks, codes, info, stat_s, stat_r, sel_s, rows, part_s, part_r, own_part,
    act, made_s, made_r, mix_s, mix_r,
    w_sem, shift_ss, shift_rs, code_ss, code_rs, block_ss, block_rs, info_ss, info_rs, stat_ss, stat_rs,
    sel_ss, sel_rs, part_ss, part_rs, act_ss, act_rs, made_ss, made_rs, mix_ss, mix_rs,
):
    np_, nz, nx, nt, tok, cap, experts, width = cfg
    quarter = stream.shape[-1]
    ff = w_up.shape[-1]
    fq = ff // nt
    p = lax.axis_index("pipe")
    e = lax.axis_index("expert")
    t = lax.axis_index("tensor")
    z, x = e // nx, e % nx
    n1, n2 = (nx, nz), (nz, nx)
    c1, c2 = (x, z), (z, x)

    def at1(d, j):
        return z * nx + j if d == 0 else j * nx + x

    def at2(d, j):
        return j * nx + x if d == 0 else z * nx + j

    def to_expert(j):
        return {"expert": j}

    started = []

    def copy(src, dst, ss, rs, dev):
        c = pltpu.make_async_remote_copy(
            src_ref=src, dst_ref=dst, send_sem=ss, recv_sem=rs, device_id=dev, device_id_type=MESH
        )
        return c

    def send(*a):
        c = copy(*a)
        c.start()
        started.append(c)

    cu = pltpu.make_async_copy(w_up, up, w_sem.at[0])
    cd = pltpu.make_async_copy(w_down, down, w_sem.at[1])
    cu.start()
    cd.start()

    barrier = pltpu.get_barrier_semaphore()
    peers = [{"pipe": lax.rem(p + 1, np_)}, {"pipe": lax.rem(p + np_ - 1, np_)}]
    peers += [to_expert(at1(0, lax.rem(x + k, nx))) for k in range(1, nx)]
    peers += [to_expert(at2(0, lax.rem(z + k, nz))) for k in range(1, nz)]
    peers += [{"tensor": lax.rem(t + k, nt)} for k in range(1, nt)]
    for dev in peers:
        pl.semaphore_signal(barrier, inc=1, device_id=dev, device_id_type=MESH)

    lane = lax.broadcasted_iota(jnp.int32, (tok, LANES), 1)
    before = (
        lax.broadcasted_iota(jnp.int32, (tok, tok), 0) > lax.broadcasted_iota(jnp.int32, (tok, tok), 1)
    ).astype(F32)
    named = []
    for d in range(2):
        chosen = ids[d, 0]
        hot = jnp.zeros((tok, LANES), F32)
        for k in range(chosen.shape[1]):
            hot = hot + (chosen[:, k : k + 1] == lane).astype(F32)
        named.append(hot)
        earlier = mm(before.astype(BF), hot.astype(BF))
        codes[d, c1[d]] = (hot * (earlier + 1.0)).astype(BF)
    for i, part in enumerate(split3(router[0])):
        rparts[:, i * experts : (i + 1) * experts] = part

    pl.semaphore_wait(barrier, len(peers))

    for d in range(2):
        dev = {"pipe": lax.rem(p + (1 if d == 0 else np_ - 1), np_)}
        send(stream.at[d, 0], arr.at[d], shift_ss.at[d], shift_rs.at[d], dev)
    for d in range(2):
        for k in range(1, n1[d]):
            j = lax.rem(c1[d] + k, n1[d])
            here = codes.at[d, c1[d]]
            send(here, here, code_ss.at[d, k], code_rs.at[d, k], to_expert(at1(d, j)))
    for d in range(2):
        copy(stream.at[d, 0], arr.at[d], shift_ss.at[d], shift_rs.at[d], {"pipe": p}).wait_recv()
        for k in range(1, n1[d]):
            j = lax.rem(c1[d] + k, n1[d])
            send(arr.at[d], blocks.at[d, c1[d]], block_ss.at[d, k], block_rs.at[d, k], to_expert(at1(d, j)))
        blocks[d, c1[d]] = arr[d]

    both = jnp.concatenate([arr[0], arr[1]], axis=0).astype(F32)
    squares = jnp.sum(both * both, axis=-1, keepdims=True)
    scaled = both * gain[...]
    hi, mid, low = split3(scaled)
    n = 2 * tok
    prod = mm(jnp.concatenate([hi, mid, low], axis=0), rparts[...])
    r0, r1, r2 = (slice(i * experts, (i + 1) * experts) for i in range(3))
    small = prod[2 * n :, r0] + prod[n : 2 * n, r1] + prod[:n, r2]
    partial = prod[:n, r0] + (prod[:n, r1] + prod[n : 2 * n, r0] + small)
    stat_s[:, :experts] = partial
    stat_s[:, experts:] = jnp.broadcast_to(squares, (n, LANES - experts))
    for k in range(1, nt):
        send(stat_s, stat_r.at[k], stat_ss.at[k], stat_rs.at[k], {"tensor": lax.rem(t + k, nt)})
    total = stat_s[...]
    for k in range(1, nt):
        copy(stat_s, stat_r.at[k], stat_ss.at[k], stat_rs.at[k], {"tensor": t}).wait_recv()
        total = total + stat_r[k]
    inverse = lax.rsqrt(total[:, experts : experts + 1] / width + norm_eps)
    hot = jnp.concatenate(named, axis=0)
    scores = jax.nn.sigmoid(total * inverse) * hot
    gates = route_scale * scores / jnp.sum(scores, axis=-1, keepdims=True)
    lane2 = lax.broadcasted_iota(jnp.int32, (n, LANES), 1)
    both_info = jnp.where(lane2 < experts, gates, jnp.broadcast_to(inverse, (n, LANES)))
    for d in range(2):
        info[d, c1[d]] = both_info[d * tok : (d + 1) * tok]
        for k in range(1, n1[d]):
            j = lax.rem(c1[d] + k, n1[d])
            here = info.at[d, c1[d]]
            send(here, here, info_ss.at[d, k], info_rs.at[d, k], to_expert(at1(d, j)))

    weights = []
    for d in range(2):
        a, b = n1[d], n2[d]
        nr, nc, per = a * b * cap, a * tok, a * cap
        for k in range(1, a):
            j = lax.rem(c1[d] + a - k, a)
            copy(codes.at[d, j], codes.at[d, j], code_ss.at[d, k], code_rs.at[d, k], to_expert(e)).wait_recv()
        code = codes[d].reshape(nc, LANES)
        rr = lax.broadcasted_iota(jnp.int32, (nr, LANES), 0)
        at = at2(d, over(rr, per, nr))
        pick = (lax.broadcasted_iota(jnp.int32, (nr, LANES), 1) == at).astype(F32).astype(BF)

        def chosen_of(shape, rdim, value):
            r = lax.broadcasted_iota(jnp.int32, shape, rdim)
            c = lax.broadcasted_iota(jnp.int32, shape, 1 - rdim)
            third = over(r, cap, nr)
            slot = r - third * cap
            block = third - over(r, per, nr) * a
            return (value == (slot + 1).astype(F32)) & (block == over(c, tok, nc))

        sel = chosen_of((nr, nc), 0, nt_dot(pick, code)).astype(F32).astype(BF)
        keep = chosen_of((nc, nr), 1, nt_dot(code, pick))
        for k in range(1, a):
            j = lax.rem(c1[d] + a - k, a)
            copy(info.at[d, j], info.at[d, j], info_ss.at[d, k], info_rs.at[d, k], to_expert(e)).wait_recv()
        facts = info[d].reshape(nc, LANES)
        ghi = facts.astype(BF)
        glo = (facts - ghi.astype(F32)).astype(BF)
        whi = jnp.where(keep, nt_dot(ghi, pick), 0.0).astype(BF)
        wlo = jnp.where(keep, nt_dot(glo, pick), 0.0).astype(BF)
        weights.append((whi, wlo))
        for k in range(1, a):
            j = lax.rem(c1[d] + a - k, a)
            copy(arr.at[d], blocks.at[d, j], block_ss.at[d, k], block_rs.at[d, k], to_expert(e)).wait_recv()
        inv = facts[:, experts : experts + 1]
        hidden = (blocks[d].reshape(nc, quarter).astype(F32) * gain[...] * inv).astype(BF)
        picked = mm(sel, hidden)
        for j in range(b):
            sel_s[d, j] = picked[j * per : (j + 1) * per].astype(BF)
        for k in range(1, b):
            j = lax.rem(c2[d] + k, b)
            send(sel_s.at[d, j], rows.at[d, c2[d]], sel_ss.at[d, k], sel_rs.at[d, k], to_expert(at2(d, j)))
        rows[d, c2[d]] = sel_s[d, c2[d]]

    cu.wait()
    for d in range(2):
        a, b = n1[d], n2[d]
        nr = a * b * cap
        for k in range(1, b):
            j = lax.rem(c2[d] + b - k, b)
            copy(sel_s.at[d, j], rows.at[d, j], sel_ss.at[d, k], sel_rs.at[d, k], to_expert(e)).wait_recv()
        lhs = rows[d].reshape(nr, quarter)
        for k in list(range(1, nt)) + [0]:
            q = lax.rem(t + k, nt)
            part = mm(lhs, up[:, pl.ds(pl.multiple_of(q * fq, fq), fq)])
            if k:
                part_s[d, k] = part.astype(BF)
                send(part_s.at[d, k], part_r.at[d, k], part_ss.at[d, k], part_rs.at[d, k], {"tensor": q})
            else:
                own_part[d] = part
    for d in range(2):
        inner = own_part[d]
        for k in range(1, nt):
            copy(part_s.at[d, k], part_r.at[d, k], part_ss.at[d, k], part_rs.at[d, k], {"tensor": t}).wait_recv()
            inner = inner + part_r[d, k].astype(F32)
        act[d, t] = jax.nn.silu(inner).astype(BF)
        for k in range(1, nt):
            q = lax.rem(t + k, nt)
            send(act.at[d, t], act.at[d, t], act_ss.at[d, k], act_rs.at[d, k], {"tensor": q})
    cd.wait()
    for d in range(2):
        a, b = n1[d], n2[d]
        per = a * cap
        for k in range(1, nt):
            q = lax.rem(t + nt - k, nt)
            copy(act.at[d, q], act.at[d, q], act_ss.at[d, k], act_rs.at[d, k], {"tensor": t}).wait_recv()
        lhs = jnp.concatenate([act[d, q] for q in range(nt)], axis=1)
        step = min(256, quarter)
        for s in range(0, quarter, step):
            made = mm(lhs, down[:, s : s + step])
            for j in range(b):
                made_s[d, j, :, s : s + step] = made[j * per : (j + 1) * per].astype(BF)
        for k in range(1, b):
            j = lax.rem(c2[d] + k, b)
            send(made_s.at[d, j], made_r.at[d, c2[d]], made_ss.at[d, k], made_rs.at[d, k], to_expert(at2(d, j)))
        made_r[d, c2[d]] = made_s[d, c2[d]]

    for d in range(2):
        a, b = n1[d], n2[d]
        nr = a * b * cap
        for k in range(1, b):
            j = lax.rem(c2[d] + b - k, b)
            copy(made_s.at[d, j], made_r.at[d, j], made_ss.at[d, k], made_rs.at[d, k], to_expert(e)).wait_recv()
        back = made_r[d].reshape(nr, quarter)
        whi, wlo = weights[d]
        mixed = mm(whi, back) + mm(wlo, back)
        for j in range(a):
            mix_s[d, j] = mixed[j * tok : (j + 1) * tok].astype(BF)
        for k in range(1, a):
            j = lax.rem(c1[d] + k, a)
            send(mix_s.at[d, j], mix_r.at[d, k], mix_ss.at[d, k], mix_rs.at[d, k], to_expert(at1(d, j)))
    for d in range(2):
        total = mix_s[d, c1[d]].astype(F32)
        for k in range(1, n1[d]):
            copy(mix_s.at[d, 0], mix_r.at[d, k], mix_ss.at[d, k], mix_rs.at[d, k], to_expert(e)).wait_recv()
            total = total + mix_r[d, k].astype(F32)
        out[d, 0] = (arr[d].astype(F32) + total).astype(BF)
    for c in started:
        c.wait_send()


def solution(mesh, nz=8, nx=8, cap=3):
    np_, nt = mesh.shape["pipe"], mesh.shape["tensor"]

    def shards(stream, ids, gain, router, w_up, w_down):
        tok, quarter = stream.shape[2:]
        experts, ff = router.shape[2], w_up.shape[2]
        cfg = (np_, nz, nx, nt, tok, cap, experts, float(quarter * nt))
        big, per = max(nz, nx), (nx * cap, nz * cap)
        assert nx == nz
        nr, fq = nx * nz * cap, ff // nt
        V, S = pltpu.VMEM, pltpu.SemaphoreType.DMA
        whole = pl.BlockSpec(memory_space=V)
        far = pl.BlockSpec(memory_space=pl.ANY)
        vmem = [
            V((quarter, ff), BF), V((ff, quarter), BF), V((quarter, 3 * experts), BF),
            V((2, tok, quarter), BF), V((2, big, tok, quarter), BF), V((2, big, tok, LANES), BF), V((2, big, tok, LANES), F32),
            V((2 * tok, LANES), F32), V((nt, 2 * tok, LANES), F32),
            V((2, big, per[0], quarter), BF), V((2, big, per[0], quarter), BF),
            V((2, nt, nr, fq), BF), V((2, nt, nr, fq), BF), V((2, nr, fq), F32), V((2, nt, nr, fq), BF),
            V((2, big, per[0], quarter), BF), V((2, big, per[0], quarter), BF),
            V((2, big, tok, quarter), BF), V((2, big, tok, quarter), BF),
        ]
        sems = [S((2,)), S((2,)), S((2,))] + [S((2, big))] * 6 + [S((nt,))] * 2 + [S((2, big))] * 2 + [S((2, nt))] * 4 + [S((2, big))] * 4
        return pl.pallas_call(
            functools.partial(layer, cfg),
            out_shape=jax.ShapeDtypeStruct(stream.shape, BF),
            in_specs=[whole] * 4 + [far] * 2,
            out_specs=whole,
            scratch_shapes=vmem + sems,
            compiler_params=pltpu.CompilerParams(
                collective_id=0, has_side_effects=True, vmem_limit_bytes=48 * 1024 * 1024
            ),
        )(stream, ids, gain, router, w_up[0], w_down[0])

    return jax.shard_map(
        shards,
        mesh=mesh,
        in_specs=(
            P(None, "pipe", "expert", "tensor"),
            P(None, "pipe", "expert", None),
            P("pipe", "tensor"),
            P("pipe", "tensor", None),
            P("expert", "tensor", None),
            P("expert", None, "tensor"),
        ),
        out_specs=P(None, "pipe", "expert", "tensor"),
        check_vma=False,
    )
```

```python
import functools

import jax
import jax.numpy as jnp
from jax import lax
from jax.experimental import pallas as pl
from jax.experimental.pallas import tpu as pltpu
from jax.sharding import PartitionSpec as P

norm_eps = 1e-06
route_scale = 2.5
MESH = pl.DeviceIdType.MESH
BF = jnp.bfloat16
F32 = jnp.float32
LANES = 128


def over(v, n, limit):
    m = -(-65536 // n)
    assert all((i * m) >> 16 == i // n for i in range(limit))
    return (v * m) >> 16


def split3(v):
    hi = v.astype(BF)
    rest = v - hi.astype(F32)
    mid = rest.astype(BF)
    low = (rest - mid.astype(F32)).astype(BF)
    return hi, mid, low


def nt_dot(a, b):
    return lax.dot_general(a, b, (((1,), (1,)), ((), ())), preferred_element_type=F32)


def ahead(n):
    return sorted(range(1, n), key=lambda k: -min(k, n - k))


def groups(n):
    near = [k for k in range(n) if min(k, n - k) <= n // 4]
    return [near, [k for k in range(n) if k not in near]]


def mm(a, b):
    return jnp.dot(a, b, preferred_element_type=F32)


def layer(
    cfg, stream_h, ids_h, gain_h, router_h, w_up, w_down, out,
    stream, ids, gain, router, up, down, rparts, arr, blocks, codes, info, stat_s, stat_r, sel_s, rows, far_part, own_part,
    over_s, over_r, pair_s, pair_r, cross_r, act, made_s, made_r, mix_s, mix_r,
    w_sem, shift_ss, shift_rs, code_ss, code_rs, block_ss, block_rs, info_ss, info_rs, stat_ss, stat_rs,
    sel_ss, sel_rs, over_ss, over_rs, pair_ss, pair_rs, cross_rs, act_ss, act_rs, made_ss, made_rs, mix_ss, mix_rs,
):
    np_, nz, nx, nt, tok, cap, experts, width = cfg
    quarter = stream.shape[-1]
    ff = w_up.shape[-1]
    fq = ff // nt
    p = lax.axis_index("pipe")
    e = lax.axis_index("expert")
    t = lax.axis_index("tensor")
    z, x = e // nx, e % nx
    n1, n2 = (nx, nz), (nz, nx)
    c1, c2 = (x, z), (z, x)

    parts = groups(nx)
    sizes = [2 * len(ks) for ks in parts]
    firsts = [0, sizes[0]]
    per = nx * cap
    place = {}
    for g in range(2):
        for d in range(2):
            for i, k in enumerate(parts[g]):
                place[d, k] = firsts[g] + d * len(parts[g]) + i
    spans = [pl.ds(firsts[g] * per, sizes[g] * per) for g in range(2)]

    def at1(d, j):
        return z * nx + j if d == 0 else j * nx + x

    def at2(d, j):
        return j * nx + x if d == 0 else z * nx + j

    def to_expert(j):
        return {"expert": j}

    started = []

    def copy(src, dst, ss, rs, dev):
        c = pltpu.make_async_remote_copy(
            src_ref=src, dst_ref=dst, send_sem=ss, recv_sem=rs, device_id=dev, device_id_type=MESH
        )
        return c

    def send(*a):
        c = copy(*a)
        c.start()
        started.append(c)

    barrier = pltpu.get_barrier_semaphore()
    peers = [{"pipe": lax.rem(p + 1, np_)}, {"pipe": lax.rem(p + np_ - 1, np_)}]
    peers += [to_expert(at1(0, lax.rem(x + k, nx))) for k in range(1, nx)]
    peers += [to_expert(at2(0, lax.rem(z + k, nz))) for k in range(1, nz)]
    peers += [{"tensor": lax.rem(t + k, nt)} for k in range(1, nt)]
    for dev in peers:
        pl.semaphore_signal(barrier, inc=1, device_id=dev, device_id_type=MESH)
    loads = [
        pltpu.make_async_copy(a, b, w_sem.at[i])
        for i, (a, b) in enumerate(
            [(ids_h, ids), (stream_h, stream), (gain_h, gain), (router_h, router), (w_up, up), (w_down, down)]
        )
    ]
    for c in loads:
        c.start()
    cu, cd = loads[4:]

    loads[0].wait()
    row = lax.broadcasted_iota(jnp.int32, (LANES, tok), 0)
    ti = lax.broadcasted_iota(jnp.int32, (tok, tok), 0)
    tj = lax.broadcasted_iota(jnp.int32, (tok, tok), 1)
    before = (ti > tj).astype(F32).astype(BF)
    same = (ti == tj).astype(F32).astype(BF)
    named = []
    for d in range(2):
        chosen = ids[d, 0]
        turned = jnp.zeros((LANES, tok), F32)
        for k in range(chosen.shape[0]):
            turned = turned + (chosen[k : k + 1] == row).astype(F32)
        turned = turned.astype(BF)
        hot = nt_dot(same, turned)
        earlier = nt_dot(before, turned)
        named.append(hot)
        codes[d, c1[d]] = (hot * (earlier + 1.0)).astype(BF)
    loads[1].wait()
    loads[2].wait()
    loads[3].wait()
    for i, part in enumerate(split3(router[0] * gain[...])):
        rparts[i * experts : (i + 1) * experts] = part

    pl.semaphore_wait(barrier, len(peers))

    for d in range(2):
        dev = {"pipe": lax.rem(p + (1 if d == 0 else np_ - 1), np_)}
        send(stream.at[d, 0], arr.at[d], shift_ss.at[d], shift_rs.at[d], dev)
    for d in range(2):
        for k in ahead(n1[d]):
            j = lax.rem(c1[d] + k, n1[d])
            here = codes.at[d, c1[d]]
            send(here, here, code_ss.at[d, k], code_rs.at[d, k], to_expert(at1(d, j)))
    for d in range(2):
        copy(stream.at[d, 0], arr.at[d], shift_ss.at[d], shift_rs.at[d], {"pipe": p}).wait_recv()
        for k in ahead(n1[d]):
            j = lax.rem(c1[d] + k, n1[d])
            send(arr.at[d], blocks.at[d, c1[d]], block_ss.at[d, k], block_rs.at[d, k], to_expert(at1(d, j)))
        blocks[d, c1[d]] = arr[d]

    raw = jnp.concatenate([arr[0], arr[1]], axis=0)
    both = raw.astype(F32)
    squares = jnp.sum(both * both, axis=-1, keepdims=True)
    n = 2 * tok
    prod = nt_dot(raw, rparts[...])
    partial = prod[:, :experts] + (prod[:, experts : 2 * experts] + prod[:, 2 * experts : 3 * experts])
    stat_s[:, :experts] = partial
    stat_s[:, experts:] = jnp.broadcast_to(squares, (n, LANES - experts))
    for k in range(1, nt):
        send(stat_s, stat_r.at[k], stat_ss.at[k], stat_rs.at[k], {"tensor": lax.rem(t + k, nt)})
    total = stat_s[...]
    for k in range(1, nt):
        copy(stat_s, stat_r.at[k], stat_ss.at[k], stat_rs.at[k], {"tensor": t}).wait_recv()
        total = total + stat_r[k]
    inverse = lax.rsqrt(total[:, experts : experts + 1] / width + norm_eps)
    hot = jnp.concatenate(named, axis=0)
    scores = jax.nn.sigmoid(total * inverse) * hot
    gates = route_scale * scores / jnp.sum(scores, axis=-1, keepdims=True)
    lane2 = lax.broadcasted_iota(jnp.int32, (n, LANES), 1)
    both_info = jnp.where(lane2 < experts, gates, jnp.broadcast_to(inverse, (n, LANES)))
    for d in range(2):
        info[d, c1[d]] = both_info[d * tok : (d + 1) * tok]
        for k in ahead(n1[d]):
            j = lax.rem(c1[d] + k, n1[d])
            here = info.at[d, c1[d]]
            send(here, here, info_ss.at[d, k], info_rs.at[d, k], to_expert(at1(d, j)))

    weights = []
    for d in range(2):
        a, b = n1[d], n2[d]
        nr, nc = a * b * cap, a * tok
        for k in range(1, a):
            j = lax.rem(c1[d] + a - k, a)
            copy(codes.at[d, j], codes.at[d, j], code_ss.at[d, k], code_rs.at[d, k], to_expert(e)).wait_recv()
        code = codes[d].reshape(nc, LANES)
        rr = lax.broadcasted_iota(jnp.int32, (nr, LANES), 0)
        at = at2(d, over(rr, per, nr))
        pick = (lax.broadcasted_iota(jnp.int32, (nr, LANES), 1) == at).astype(F32).astype(BF)

        def chosen_of(shape, rdim, value):
            r = lax.broadcasted_iota(jnp.int32, shape, rdim)
            c = lax.broadcasted_iota(jnp.int32, shape, 1 - rdim)
            third = over(r, cap, nr)
            slot = r - third * cap
            block = third - over(r, per, nr) * a
            return (value == (slot + 1).astype(F32)) & (block == over(c, tok, nc))

        sel = chosen_of((nr, nc), 0, nt_dot(pick, code)).astype(F32).astype(BF)
        keep = chosen_of((nc, nr), 1, nt_dot(code, pick))
        for k in range(1, a):
            j = lax.rem(c1[d] + a - k, a)
            copy(info.at[d, j], info.at[d, j], info_ss.at[d, k], info_rs.at[d, k], to_expert(e)).wait_recv()
        facts = info[d].reshape(nc, LANES)
        ghi = facts.astype(BF)
        glo = (facts - ghi.astype(F32)).astype(BF)
        whi = jnp.where(keep, nt_dot(ghi, pick), 0.0).astype(BF)
        wlo = jnp.where(keep, nt_dot(glo, pick), 0.0).astype(BF)
        weights.append((whi, wlo))
        for k in range(1, a):
            j = lax.rem(c1[d] + a - k, a)
            copy(arr.at[d], blocks.at[d, j], block_ss.at[d, k], block_rs.at[d, k], to_expert(e)).wait_recv()
        inv = facts[:, experts : experts + 1]
        hidden = (blocks[d].reshape(nc, quarter).astype(F32) * gain[...] * inv).astype(BF)
        picked = mm(sel, hidden)
        for j in range(b):
            sel_s[d, j] = picked[j * per : (j + 1) * per].astype(BF)
    for g in range(2):
        for k in ahead(n2[0]):
            if k in parts[g]:
                for d in range(2):
                    j = lax.rem(c2[d] + k, n2[d])
                    send(sel_s.at[d, j], rows.at[place[d, k]], sel_ss.at[d, k], sel_rs.at[d, k], to_expert(at2(d, j)))
    for d in range(2):
        rows[place[d, 0]] = sel_s[d, c2[d]]

    end = (t == 0) | (t == nt - 1)
    pair = t + 1 - 2 * (t % 2)
    flip, turn = nt - 1 - t, lax.rem(t + 2, nt)
    far_end = jnp.where(end, flip, turn)
    far_mid = jnp.where(end, turn, flip)

    def columns(q):
        return up[:, pl.ds(pl.multiple_of(q * fq, fq), fq)]

    def over_copy(g):
        o = over_s.at[:, spans[g]]
        return copy(o, over_r.at[:, spans[g]], over_ss.at[g, 0], over_rs.at[g], {"tensor": pair})

    def pair_copy(g):
        return copy(pair_s.at[spans[g]], pair_r.at[spans[g]], pair_ss.at[g], pair_rs.at[g], {"tensor": pair})

    def cross_copy(g, i, q):
        return copy(over_s.at[i, spans[g]], cross_r.at[spans[g]], over_ss.at[g, i], cross_rs.at[g], {"tensor": q})

    def act_copy(g, q, i, o, to):
        c = act.at[q, spans[g]]
        return copy(c, c, act_ss.at[g, o], act_rs.at[g, i], {"tensor": to})

    def go(c):
        c.start()
        started.append(c)

    def arrive(g):
        for d in range(2):
            for k in parts[g]:
                if k:
                    copy(sel_s.at[d, 0], rows.at[place[d, k]], sel_ss.at[d, k], sel_rs.at[d, k], to_expert(e)).wait_recv()

    def upward(g):
        count = sizes[g]
        lhs = rows[firsts[g] : firsts[g] + count].reshape(count * per, quarter)
        for i, q in enumerate((far_end, far_mid)):
            far_part[i, spans[g]] = mm(lhs, columns(q))

        @pl.when(end)
        def _():
            over_s[:, spans[g]] = far_part[:, spans[g]].astype(BF)
            over_copy(g).start()

        pair_s[spans[g]] = mm(lhs, columns(pair)).astype(BF)
        go(pair_copy(g))
        own_part[spans[g]] = mm(lhs, columns(t))

    def combine(g):
        @pl.when(jnp.logical_not(end))
        def _():
            over_copy(g).wait_recv()
            over_s[:, spans[g]] = (far_part[:, spans[g]] + over_r[:, spans[g]].astype(F32)).astype(BF)
            cross_copy(g, 0, far_end).start()
            cross_copy(g, 1, far_mid).start()

    def activate(g):
        pair_copy(g).wait_recv()
        cross_copy(g, 0, t).wait_recv()
        inner = own_part[spans[g]] + pair_r[spans[g]].astype(F32) + cross_r[spans[g]].astype(F32)
        act[t, spans[g]] = jax.nn.silu(inner).astype(BF)

        @pl.when(end)
        def _():
            act_copy(g, t, 2, 1, far_mid).start()

        @pl.when(jnp.logical_not(end))
        def _():
            act_copy(g, t, 1, 1, far_mid).start()

        go(act_copy(g, t, 0, 0, pair))

    def relay(g):
        @pl.when(jnp.logical_not(end))
        def _():
            act_copy(g, far_mid, 1, 2, t).wait_recv()
            act_copy(g, far_mid, 1, 2, pair).start()
            act_copy(g, far_end, 2, 3, t).wait_recv()
            act_copy(g, far_end, 2, 3, pair).start()

    def downward(g):
        act_copy(g, pair, 0, 0, t).wait_recv()

        @pl.when(end)
        def _():
            act_copy(g, far_mid, 1, 2, t).wait_recv()
            act_copy(g, far_end, 2, 3, t).wait_recv()

        lhs = jnp.concatenate([act[q, spans[g]] for q in range(nt)], axis=1)
        step = min(256, quarter)
        for s in range(0, quarter, step):
            made = mm(lhs, down[:, s : s + step])
            for j in range(sizes[g]):
                made_s[firsts[g] + j, :, s : s + step] = made[j * per : (j + 1) * per].astype(BF)
        for k in sorted(parts[g], key=lambda k: -min(k, n2[0] - k)):
            for d in range(2):
                here = made_s.at[place[d, k]]
                if k:
                    j = lax.rem(c2[d] + n2[d] - k, n2[d])
                    send(here, made_r.at[d, c2[d]], made_ss.at[d, k], made_rs.at[d, k], to_expert(at2(d, j)))
                else:
                    made_r[d, c2[d]] = made_s[place[d, k]]

    cu.wait()
    cd.wait()
    arrive(0)
    upward(0)
    combine(0)
    arrive(1)
    upward(1)
    activate(0)
    combine(1)
    relay(0)
    activate(1)
    downward(0)
    relay(1)
    downward(1)
    for g in range(2):
        act_copy(g, t, 1, 1, far_mid).wait_send()

        @pl.when(end)
        def _():
            over_copy(g).wait_send()

        @pl.when(jnp.logical_not(end))
        def _():
            cross_copy(g, 0, far_end).wait_send()
            cross_copy(g, 1, far_mid).wait_send()
            act_copy(g, far_mid, 1, 2, pair).wait_send()
            act_copy(g, far_end, 2, 3, pair).wait_send()

    for d in range(2):
        a, b = n1[d], n2[d]
        nr = a * b * cap
        for k in range(1, b):
            j = lax.rem(c2[d] + k, b)
            copy(made_s.at[0], made_r.at[d, j], made_ss.at[d, k], made_rs.at[d, k], to_expert(e)).wait_recv()
        back = made_r[d].reshape(nr, quarter)
        whi, wlo = weights[d]
        mixed = mm(whi, back) + mm(wlo, back)
        for j in range(a):
            mix_s[d, j] = mixed[j * tok : (j + 1) * tok].astype(BF)
        for k in ahead(a):
            j = lax.rem(c1[d] + k, a)
            send(mix_s.at[d, j], mix_r.at[d, k], mix_ss.at[d, k], mix_rs.at[d, k], to_expert(at1(d, j)))
    for d in range(2):
        total = mix_s[d, c1[d]].astype(F32)
        for k in range(1, n1[d]):
            copy(mix_s.at[d, 0], mix_r.at[d, k], mix_ss.at[d, k], mix_rs.at[d, k], to_expert(e)).wait_recv()
            total = total + mix_r[d, k].astype(F32)
        out[d, 0] = (arr[d].astype(F32) + total).astype(BF)
    for c in started:
        c.wait_send()


def solution(mesh, nz=8, nx=8, cap=3):
    np_, nt = mesh.shape["pipe"], mesh.shape["tensor"]

    def shards(stream, ids, gain, router, w_up, w_down):
        tok, quarter = stream.shape[2:]
        experts, ff = router.shape[2], w_up.shape[2]
        cfg = (np_, nz, nx, nt, tok, cap, experts, float(quarter * nt))
        big, per = max(nz, nx), (nx * cap, nz * cap)
        assert nx == nz
        nr, fq = nx * nz * cap, ff // nt
        V, S = pltpu.VMEM, pltpu.SemaphoreType.DMA
        whole = pl.BlockSpec(memory_space=V)
        far = pl.BlockSpec(memory_space=pl.ANY)
        vmem = [
            V(stream.shape, BF), V((2, 1, ids.shape[3], tok), jnp.int32), V(gain.shape, F32), V((1, experts, quarter), F32),
            V((quarter, ff), BF), V((ff, quarter), BF), V((3 * experts, quarter), BF),
            V((2, tok, quarter), BF), V((2, big, tok, quarter), BF), V((2, big, tok, LANES), BF), V((2, big, tok, LANES), F32),
            V((2 * tok, LANES), F32), V((nt, 2 * tok, LANES), F32),
            V((2, big, per[0], quarter), BF), V((2 * big, per[0], quarter), BF),
            V((2, 2 * nr, fq), F32), V((2 * nr, fq), F32),
            V((2, 2 * nr, fq), BF), V((2, 2 * nr, fq), BF), V((2 * nr, fq), BF), V((2 * nr, fq), BF), V((2 * nr, fq), BF),
            V((nt, 2 * nr, fq), BF),
            V((2 * big, per[0], quarter), BF), V((2, big, per[0], quarter), BF),
            V((2, big, tok, quarter), BF), V((2, big, tok, quarter), BF),
        ]
        sems = [S((6,)), S((2,)), S((2,))] + [S((2, big))] * 6 + [S((nt,))] * 2 + [S((2, big))] * 2 + [S((2, 2))] + [S((2,))] * 4 + [S((2, 4))] * 2 + [S((2, big))] * 4
        return pl.pallas_call(
            functools.partial(layer, cfg),
            out_shape=jax.ShapeDtypeStruct(stream.shape, BF),
            in_specs=[far] * 6,
            out_specs=whole,
            scratch_shapes=vmem + sems,
            compiler_params=pltpu.CompilerParams(
                collective_id=0, has_side_effects=True, vmem_limit_bytes=67043328
            ),
        )(stream, jnp.swapaxes(ids, 2, 3), gain, jnp.swapaxes(router, 1, 2), w_up[0], w_down[0])

    return jax.shard_map(
        shards,
        mesh=mesh,
        in_specs=(
            P(None, "pipe", "expert", "tensor"),
            P(None, "pipe", "expert", None),
            P("pipe", "tensor"),
            P("pipe", "tensor", None),
            P("expert", "tensor", None),
            P("expert", None, "tensor"),
        ),
        out_specs=P(None, "pipe", "expert", "tensor"),
        check_vma=False,
    )
```

```python
import functools

import jax
import jax.numpy as jnp
from jax import lax
from jax.experimental import pallas as pl
from jax.experimental.pallas import tpu as pltpu
from jax.sharding import PartitionSpec as P

norm_eps = 1e-06
route_scale = 2.5
tree = (True, True, True)
passed = (True, True, False)
MESH = pl.DeviceIdType.MESH
BF = jnp.bfloat16
F32 = jnp.float32
LANES = 128


def over(v, n, limit):
    m = -(-65536 // n)
    assert all((i * m) >> 16 == i // n for i in range(limit))
    return (v * m) >> 16


def split3(v):
    hi = v.astype(BF)
    rest = v - hi.astype(F32)
    mid = rest.astype(BF)
    low = (rest - mid.astype(F32)).astype(BF)
    return hi, mid, low


def nt_dot(a, b):
    return lax.dot_general(a, b, (((1,), (1,)), ((), ())), preferred_element_type=F32)


def ahead(n):
    return sorted(range(1, n), key=lambda k: -min(k, n - k))


def groups(n):
    edge = n // 8
    away = [min(k, n - k) for k in range(n)]
    return [
        [k for k in range(n) if away[k] > edge + 1],
        [k for k in range(n) if away[k] <= edge],
        [k for k in range(n) if away[k] == edge + 1],
    ]


def mm(a, b):
    return jnp.dot(a, b, preferred_element_type=F32)


def layer(
    cfg, stream_h, ids_h, gain_h, router_h, w_up, w_down, out,
    stream, ids, gain, router, up, down, rparts, arr, blocks, codes, info, stat_s, stat_r, hots, mixers, sel_s, rows, far_part, own_part,
    over_s, over_r, pair_s, pair_r, cross_r, act, made_s, made_r, mix_s, mix_r,
    w_sem, shift_ss, shift_rs, code_ss, code_rs, block_ss, block_rs, info_ss, info_rs, stat_ss, stat_rs,
    sel_ss, sel_rs, over_ss, over_rs, pair_ss, pair_rs, cross_rs, act_ss, act_rs, made_ss, made_rs, mix_ss, mix_rs,
):
    np_, nz, nx, nt, tok, cap, experts, width = cfg
    quarter = stream.shape[-1]
    ff = w_up.shape[-1]
    fq = ff // nt
    p = lax.axis_index("pipe")
    e = lax.axis_index("expert")
    t = lax.axis_index("tensor")
    z, x = e // nx, e % nx
    n1, n2 = (nx, nz), (nz, nx)
    c1, c2 = (x, z), (z, x)

    def coord1(d):
        return x + d * (z - x)

    def coord2(d):
        return z + d * (x - z)

    parts = groups(nx)
    sizes = [2 * len(ks) for ks in parts]
    firsts = [sum(sizes[:g]) for g in range(3)]
    per = nx * cap
    place = {}
    for g in range(3):
        for d in range(2):
            for i, k in enumerate(parts[g]):
                place[d, k] = firsts[g] + d * len(parts[g]) + i
    spans = [pl.ds(firsts[g] * per, sizes[g] * per) for g in range(3)]

    def at1(d, j):
        return z * nx + j + d * (j * nx + x - z * nx - j)

    def at2(d, j):
        return j * nx + x + d * (z * nx + j - j * nx - x)

    def to_expert(j):
        return {"expert": j}

    started = []

    def copy(src, dst, ss, rs, dev):
        c = pltpu.make_async_remote_copy(
            src_ref=src, dst_ref=dst, send_sem=ss, recv_sem=rs, device_id=dev, device_id_type=MESH
        )
        return c

    def send(*a):
        c = copy(*a)
        c.start()
        started.append(c)

    barrier = pltpu.get_barrier_semaphore()
    peers = [{"pipe": lax.rem(p + 1, np_)}, {"pipe": lax.rem(p + np_ - 1, np_)}]
    peers += [to_expert(at1(0, lax.rem(x + k, nx))) for k in range(1, nx)]
    peers += [to_expert(at2(0, lax.rem(z + k, nz))) for k in range(1, nz)]
    peers += [{"tensor": lax.rem(t + k, nt)} for k in range(1, nt)]
    for dev in peers:
        pl.semaphore_signal(barrier, inc=1, device_id=dev, device_id_type=MESH)
    loads = [
        pltpu.make_async_copy(a, b, w_sem.at[i])
        for i, (a, b) in enumerate(
            [(ids_h, ids), (stream_h, stream), (gain_h, gain), (router_h, router), (w_up, up), (w_down, down)]
        )
    ]
    for c in loads:
        c.start()
    cu, cd = loads[4:]

    loads[0].wait()
    lane = lax.broadcasted_iota(jnp.int32, (tok, LANES), 1)
    row = lax.broadcasted_iota(jnp.int32, (LANES, tok), 0)
    ti = lax.broadcasted_iota(jnp.int32, (tok, tok), 0)
    tj = lax.broadcasted_iota(jnp.int32, (tok, tok), 1)
    before = (ti > tj).astype(F32).astype(BF)
    same = (ti == tj).astype(F32).astype(BF)
    for d in range(2):
        chosen = ids[d, 0]
        turned = jnp.zeros((LANES, tok), F32)
        for k in range(chosen.shape[0]):
            turned = turned + (chosen[k : k + 1] == row).astype(F32)
        turned = turned.astype(BF)
        hot = nt_dot(same, turned)
        earlier = nt_dot(before, turned)
        hots[d] = hot
        codes[d, c1[d]] = (hot * (earlier + 1.0)).astype(BF)
    loads[1].wait()
    pl.semaphore_wait(barrier, len(peers))

    for d in range(2):
        dev = {"pipe": lax.rem(p + (1 if d == 0 else np_ - 1), np_)}
        send(stream.at[d, 0], arr.at[d], shift_ss.at[d], shift_rs.at[d], dev)
    for d in range(2):
        for k in ahead(n1[d]):
            j = lax.rem(c1[d] + k, n1[d])
            here = codes.at[d, c1[d]]
            send(here, here, code_ss.at[d, k], code_rs.at[d, k], to_expert(at1(d, j)))
    loads[2].wait()
    loads[3].wait()
    for i, part in enumerate(split3(router[0] * gain[...])):
        rparts[i * experts : (i + 1) * experts] = part

    a = nx
    first = 1 - p % 2
    for d in (first, 1 - first):
        copy(stream.at[d, 0], arr.at[d], shift_ss.at[d], shift_rs.at[d], {"pipe": p}).wait_recv()
        own = coord1(d)
        for k in ahead(a):
            j = lax.rem(own + k, a)
            send(arr.at[d], blocks.at[d, own], block_ss.at[d, k], block_rs.at[d, k], to_expert(at1(d, j)))
        raw = arr[d]
        blocks[d, own] = raw
        wide = raw.astype(F32)
        squares = jnp.sum(wide * wide, axis=-1, keepdims=True)
        prod = nt_dot(raw, rparts[...])
        partial = prod[:, :experts] + (prod[:, experts : 2 * experts] + prod[:, 2 * experts : 3 * experts])
        stat_s[d, :, :experts] = partial
        stat_s[d, :, experts:] = jnp.broadcast_to(squares, (tok, LANES - experts))
        for k in range(1, nt):
            q = lax.rem(t + k, nt)
            send(stat_s.at[d], stat_r.at[d, k], stat_ss.at[d, k], stat_rs.at[d, k], {"tensor": q})
    for d in (first, 1 - first):
        total = stat_s[d]
        for k in range(1, nt):
            copy(stat_s.at[d], stat_r.at[d, k], stat_ss.at[d, k], stat_rs.at[d, k], {"tensor": t}).wait_recv()
            total = total + stat_r[d, k]
        inverse = lax.rsqrt(total[:, experts : experts + 1] / width + norm_eps)
        scores = jax.nn.sigmoid(total * inverse) * hots[d]
        gates = route_scale * scores / jnp.sum(scores, axis=-1, keepdims=True)
        own = coord1(d)
        info[d, own] = jnp.where(lane < experts, gates, jnp.broadcast_to(inverse, (tok, LANES)))
        for k in ahead(a):
            j = lax.rem(own + k, a)
            here = info.at[d, own]
            send(here, here, info_ss.at[d, k], info_rs.at[d, k], to_expert(at1(d, j)))

    b = nx
    nr, nc = a * b * cap, a * tok
    for d in (first, 1 - first):
        own = coord1(d)
        for k in range(1, a):
            j = lax.rem(own + a - k, a)
            copy(codes.at[d, j], codes.at[d, j], code_ss.at[d, k], code_rs.at[d, k], to_expert(e)).wait_recv()
        code = codes[d].reshape(nc, LANES)
        rr = lax.broadcasted_iota(jnp.int32, (nr, LANES), 0)
        at = at2(d, over(rr, per, nr))
        pick = (lax.broadcasted_iota(jnp.int32, (nr, LANES), 1) == at).astype(F32).astype(BF)

        def chosen_of(shape, rdim, value):
            r = lax.broadcasted_iota(jnp.int32, shape, rdim)
            c = lax.broadcasted_iota(jnp.int32, shape, 1 - rdim)
            third = over(r, cap, nr)
            slot = r - third * cap
            block = third - over(r, per, nr) * a
            return (value == (slot + 1).astype(F32)) & (block == over(c, tok, nc))

        sel = chosen_of((nr, nc), 0, nt_dot(pick, code)).astype(F32).astype(BF)
        keep = chosen_of((nc, nr), 1, nt_dot(code, pick))
        for k in range(1, a):
            j = lax.rem(own + a - k, a)
            copy(info.at[d, j], info.at[d, j], info_ss.at[d, k], info_rs.at[d, k], to_expert(e)).wait_recv()
        for k in range(1, a):
            j = lax.rem(own + a - k, a)
            copy(arr.at[d], blocks.at[d, j], block_ss.at[d, k], block_rs.at[d, k], to_expert(e)).wait_recv()
        facts = info[d].reshape(nc, LANES)
        inv = facts[:, experts : experts + 1]
        hidden = (blocks[d].reshape(nc, quarter).astype(F32) * gain[...] * inv).astype(BF)
        picked = mm(sel, hidden)
        for j in range(b):
            sel_s[d, j] = picked[j * per : (j + 1) * per].astype(BF)
        over2 = coord2(d)
        for g in range(3):
            for k in ahead(b):
                if k in parts[g]:
                    j = lax.rem(over2 + k, b)
                    to = rows.at[place[0, k] + d * len(parts[g])]
                    send(sel_s.at[d, j], to, sel_ss.at[d, k], sel_rs.at[d, k], to_expert(at2(d, j)))
        rows[place[0, 0] + d * len(parts[0])] = sel_s[d, over2]
        ghi = facts.astype(BF)
        glo = (facts - ghi.astype(F32)).astype(BF)
        mixers[d, 0] = jnp.where(keep, nt_dot(ghi, pick), 0.0).astype(BF)
        mixers[d, 1] = jnp.where(keep, nt_dot(glo, pick), 0.0).astype(BF)

    end = (t == 0) | (t == nt - 1)
    pair = t + 1 - 2 * (t % 2)
    flip, turn = nt - 1 - t, lax.rem(t + 2, nt)
    far_end = jnp.where(end, flip, turn)
    far_mid = jnp.where(end, turn, flip)

    def columns(q):
        return up[:, pl.ds(pl.multiple_of(q * fq, fq), fq)]

    side = (far_end, far_mid)

    def over_copy(g, i, q):
        o = over_s.at[i, spans[g]]
        return copy(o, over_r.at[i, spans[g]], over_ss.at[g, i], over_rs.at[g, i], {"tensor": q})

    def straight_copy(g, i, o, q):
        c = over_s.at[i, spans[g]]
        return copy(c, over_r.at[o, spans[g]], over_ss.at[g, i], over_rs.at[g, o], {"tensor": q})

    def pair_copy(g):
        return copy(pair_s.at[spans[g]], pair_r.at[spans[g]], pair_ss.at[g], pair_rs.at[g], {"tensor": pair})

    def cross_copy(g, i, q):
        return copy(over_s.at[i, spans[g]], cross_r.at[spans[g]], over_ss.at[g, i], cross_rs.at[g], {"tensor": q})

    def act_copy(g, q, i, o, to):
        c = act.at[q, spans[g]]
        return copy(c, c, act_ss.at[g, o], act_rs.at[g, i], {"tensor": to})

    def go(c):
        c.start()
        started.append(c)

    def at_end(f):
        pl.when(end)(f)

    def at_mid(f):
        pl.when(jnp.logical_not(end))(f)

    def arrive(g):
        for d in range(2):
            for k in parts[g]:
                if k:
                    copy(sel_s.at[d, 0], rows.at[place[d, k]], sel_ss.at[d, k], sel_rs.at[d, k], to_expert(e)).wait_recv()

    def upward(g):
        count = sizes[g]
        lhs = rows[firsts[g] : firsts[g] + count].reshape(count * per, quarter)
        for i in range(2):
            part = mm(lhs, columns(side[i]))
            if tree[g]:
                far_part[i, spans[g]] = part

                @at_end
                def _():
                    over_s[i, spans[g]] = far_part[i, spans[g]].astype(BF)
                    over_copy(g, i, pair).start()
            else:
                over_s[i, spans[g]] = part.astype(BF)
                at_end(lambda: straight_copy(g, i, 0, side[i]).start())
                at_mid(lambda: straight_copy(g, i, 1, side[i]).start())
        pair_s[spans[g]] = mm(lhs, columns(pair)).astype(BF)
        go(pair_copy(g))
        own_part[spans[g]] = mm(lhs, columns(t))

    def combine(g):
        if tree[g]:

            @at_mid
            def _():
                for i in range(2):
                    over_copy(g, i, t).wait_recv()
                    over_s[i, spans[g]] = (far_part[i, spans[g]] + over_r[i, spans[g]].astype(F32)).astype(BF)
                    cross_copy(g, i, side[i]).start()

    def activate(g):
        pair_copy(g).wait_recv()
        inner = own_part[spans[g]] + pair_r[spans[g]].astype(F32)
        if tree[g]:
            cross_copy(g, 0, t).wait_recv()
            inner = inner + cross_r[spans[g]].astype(F32)
        else:
            for o in range(2):
                straight_copy(g, 0, o, t).wait_recv()
                inner = inner + over_r[o, spans[g]].astype(F32)
        act[t, spans[g]] = jax.nn.silu(inner).astype(BF)

        @at_end
        def _():
            if not passed[g]:
                act_copy(g, t, 2, 2, far_end).start()
            act_copy(g, t, 2, 1, far_mid).start()

        @at_mid
        def _():
            if not passed[g]:
                act_copy(g, t, 1, 2, far_end).start()
            act_copy(g, t, 1, 1, far_mid).start()

        go(act_copy(g, t, 0, 0, pair))

    def relay(g):
        if passed[g]:

            @at_mid
            def _():
                act_copy(g, far_mid, 1, 2, t).wait_recv()
                act_copy(g, far_mid, 1, 2, pair).start()
                act_copy(g, far_end, 2, 3, t).wait_recv()
                act_copy(g, far_end, 2, 3, pair).start()

    def downward(g):
        def rest():
            act_copy(g, far_mid, 1, 2, t).wait_recv()
            act_copy(g, far_end, 2, 3, t).wait_recv()

        act_copy(g, pair, 0, 0, t).wait_recv()
        if passed[g]:
            at_end(rest)
        else:
            rest()
        lhs = jnp.concatenate([act[q, spans[g]] for q in range(nt)], axis=1)
        step = min(256, quarter)
        for s in range(0, quarter, step):
            made = mm(lhs, down[:, s : s + step])
            for j in range(sizes[g]):
                made_s[firsts[g] + j, :, s : s + step] = made[j * per : (j + 1) * per].astype(BF)
        for k in sorted(parts[g], key=lambda k: -min(k, n2[0] - k)):
            for d in range(2):
                here = made_s.at[place[d, k]]
                if k:
                    j = lax.rem(c2[d] + n2[d] - k, n2[d])
                    send(here, made_r.at[d, c2[d]], made_ss.at[d, k], made_rs.at[d, k], to_expert(at2(d, j)))
                else:
                    made_r[d, c2[d]] = made_s[place[d, k]]

    cu.wait()
    arrive(0)
    upward(0)
    combine(0)
    arrive(1)
    upward(1)
    activate(0)
    combine(1)
    arrive(2)
    upward(2)
    relay(0)
    activate(1)
    combine(2)
    cd.wait()
    downward(0)
    relay(1)
    activate(2)
    downward(1)
    relay(2)
    downward(2)
    for g in range(3):
        act_copy(g, t, 1, 1, far_mid).wait_send()
        over_copy(g, 0, pair).wait_send()
        over_copy(g, 1, pair).wait_send()
        if passed[g]:

            @at_mid
            def _():
                act_copy(g, far_mid, 1, 2, pair).wait_send()
                act_copy(g, far_end, 2, 3, pair).wait_send()
        else:
            act_copy(g, t, 1, 2, far_end).wait_send()

    for d in range(2):
        a, b = n1[d], n2[d]
        nr = a * b * cap
        for k in range(1, b):
            j = lax.rem(c2[d] + k, b)
            copy(made_s.at[0], made_r.at[d, j], made_ss.at[d, k], made_rs.at[d, k], to_expert(e)).wait_recv()
        back = made_r[d].reshape(nr, quarter)
        mixed = mm(mixers[d, 0], back) + mm(mixers[d, 1], back)
        for j in range(a):
            mix_s[d, j] = mixed[j * tok : (j + 1) * tok].astype(BF)
        for k in ahead(a):
            j = lax.rem(c1[d] + k, a)
            send(mix_s.at[d, j], mix_r.at[d, k], mix_ss.at[d, k], mix_rs.at[d, k], to_expert(at1(d, j)))
    for d in range(2):
        total = mix_s[d, c1[d]].astype(F32)
        for k in range(1, n1[d]):
            copy(mix_s.at[d, 0], mix_r.at[d, k], mix_ss.at[d, k], mix_rs.at[d, k], to_expert(e)).wait_recv()
            total = total + mix_r[d, k].astype(F32)
        out[d, 0] = (arr[d].astype(F32) + total).astype(BF)
    for c in started:
        c.wait_send()


def solution(mesh, nz=8, nx=8, cap=3):
    np_, nt = mesh.shape["pipe"], mesh.shape["tensor"]

    def shards(stream, ids, gain, router, w_up, w_down):
        tok, quarter = stream.shape[2:]
        experts, ff = router.shape[2], w_up.shape[2]
        cfg = (np_, nz, nx, nt, tok, cap, experts, float(quarter * nt))
        big, per = max(nz, nx), (nx * cap, nz * cap)
        assert nx == nz
        nr, fq = nx * nz * cap, ff // nt
        V, S = pltpu.VMEM, pltpu.SemaphoreType.DMA
        whole = pl.BlockSpec(memory_space=V)
        far = pl.BlockSpec(memory_space=pl.ANY)
        vmem = [
            V(stream.shape, BF), V((2, 1, ids.shape[3], tok), jnp.int32), V(gain.shape, F32), V((1, experts, quarter), F32),
            V((quarter, ff), BF), V((ff, quarter), BF), V((3 * experts, quarter), BF),
            V((2, tok, quarter), BF), V((2, big, tok, quarter), BF), V((2, big, tok, LANES), BF), V((2, big, tok, LANES), F32),
            V((2, tok, LANES), F32), V((2, nt, tok, LANES), F32), V((2, tok, LANES), F32), V((2, 2, big * tok, nr), BF),
            V((2, big, per[0], quarter), BF), V((2 * big, per[0], quarter), BF),
            V((2, 2 * nr, fq), F32), V((2 * nr, fq), F32),
            V((2, 2 * nr, fq), BF), V((2, 2 * nr, fq), BF), V((2 * nr, fq), BF), V((2 * nr, fq), BF), V((2 * nr, fq), BF),
            V((nt, 2 * nr, fq), BF),
            V((2 * big, per[0], quarter), BF), V((2, big, per[0], quarter), BF),
            V((2, big, tok, quarter), BF), V((2, big, tok, quarter), BF),
        ]
        sems = [S((6,)), S((2,)), S((2,))] + [S((2, big))] * 6 + [S((2, nt))] * 2 + [S((2, big))] * 2 + [S((3, 2))] * 2 + [S((3,))] * 3 + [S((3, 4))] * 2 + [S((2, big))] * 4
        return pl.pallas_call(
            functools.partial(layer, cfg),
            out_shape=pltpu.VMEM(stream.shape, BF),
            in_specs=[pl.BlockSpec(memory_space=pltpu.HBM)] * 6,
            out_specs=whole,
            scratch_shapes=vmem + sems,
            compiler_params=pltpu.CompilerParams(
                collective_id=0, has_side_effects=True, vmem_limit_bytes=56 * 1024 * 1024
            ),
        )(stream, jnp.swapaxes(ids, 2, 3), gain, jnp.swapaxes(router, 1, 2), w_up[0], w_down[0])

    return jax.shard_map(
        shards,
        mesh=mesh,
        in_specs=(
            P(None, "pipe", "expert", "tensor"),
            P(None, "pipe", "expert", None),
            P("pipe", "tensor"),
            P("pipe", "tensor", None),
            P("expert", "tensor", None),
            P("expert", None, "tensor"),
        ),
        out_specs=P(None, "pipe", "expert", "tensor"),
        check_vma=False,
    )
```

```python
import functools

import jax
import jax.numpy as jnp
from jax import lax
from jax.experimental import pallas as pl
from jax.experimental.pallas import tpu as pltpu
from jax.sharding import PartitionSpec as P

norm_eps = 1e-06
route_scale = 2.5
tree = (True, True, True)
passed = (True, True, False)
MESH = pl.DeviceIdType.MESH
BF = jnp.bfloat16
F32 = jnp.float32
LANES = 128


def over(v, n, limit):
    m = -(-65536 // n)
    assert all((i * m) >> 16 == i // n for i in range(limit))
    return (v * m) >> 16


def split3(v):
    hi = v.astype(BF)
    rest = v - hi.astype(F32)
    mid = rest.astype(BF)
    low = (rest - mid.astype(F32)).astype(BF)
    return hi, mid, low


def nt_dot(a, b):
    return lax.dot_general(a, b, (((1,), (1,)), ((), ())), preferred_element_type=F32)


def ahead(n):
    return sorted(range(1, n), key=lambda k: -min(k, n - k))


def groups(n):
    edge = n // 8
    away = [min(k, n - k) for k in range(n)]
    return [
        [k for k in range(n) if away[k] > edge + 1],
        [k for k in range(n) if away[k] <= edge],
        [k for k in range(n) if away[k] == edge + 1],
    ]


def mm(a, b):
    return jnp.dot(a, b, preferred_element_type=F32)


def layer(
    cfg, stream_h, ids_h, gain_h, router_h, w_up, w_down, out,
    stream, ids, gain, router, up, down, rparts, arr, blocks, codes, info, stat_s, stat_r, hots, mixers, sel_s, rows, far_part, own_part,
    over_s, over_r, pair_s, pair_r, cross_r, act, made_s, made_r, mix_s, mix_r,
    w_sem, shift_ss, shift_rs, code_ss, code_rs, block_ss, block_rs, info_ss, info_rs, stat_ss, stat_rs,
    sel_ss, sel_rs, over_ss, over_rs, pair_ss, pair_rs, cross_rs, act_ss, act_rs, made_ss, made_rs, mix_ss, mix_rs,
):
    np_, nz, nx, nt, tok, cap, experts, width = cfg
    quarter = stream.shape[-1]
    ff = w_up.shape[-1]
    fq = ff // nt
    p = lax.axis_index("pipe")
    e = lax.axis_index("expert")
    t = lax.axis_index("tensor")
    z, x = e // nx, e % nx
    n1, n2 = (nx, nz), (nz, nx)
    c1, c2 = (x, z), (z, x)

    def coord1(d):
        return x + d * (z - x)

    def coord2(d):
        return z + d * (x - z)

    parts = groups(nx)
    sizes = [2 * len(ks) for ks in parts]
    firsts = [sum(sizes[:g]) for g in range(3)]
    per = nx * cap
    place = {}
    for g in range(3):
        for d in range(2):
            for i, k in enumerate(parts[g]):
                place[d, k] = firsts[g] + d * len(parts[g]) + i
    spans = [pl.ds(firsts[g] * per, sizes[g] * per) for g in range(3)]

    def at1(d, j):
        return z * nx + j + d * (j * nx + x - z * nx - j)

    def at2(d, j):
        return j * nx + x + d * (z * nx + j - j * nx - x)

    def to_expert(j):
        return {"expert": j}

    started = []

    def copy(src, dst, ss, rs, dev):
        c = pltpu.make_async_remote_copy(
            src_ref=src, dst_ref=dst, send_sem=ss, recv_sem=rs, device_id=dev, device_id_type=MESH
        )
        return c

    def send(*a):
        c = copy(*a)
        c.start()
        started.append(c)

    barrier = pltpu.get_barrier_semaphore()
    peers = [{"pipe": lax.rem(p + 1, np_)}, {"pipe": lax.rem(p + np_ - 1, np_)}]
    peers += [to_expert(at1(0, lax.rem(x + k, nx))) for k in range(1, nx)]
    peers += [to_expert(at2(0, lax.rem(z + k, nz))) for k in range(1, nz)]
    peers += [{"tensor": lax.rem(t + k, nt)} for k in range(1, nt)]
    for dev in peers:
        pl.semaphore_signal(barrier, inc=1, device_id=dev, device_id_type=MESH)
    loads = [
        pltpu.make_async_copy(a, b, w_sem.at[i])
        for i, (a, b) in enumerate(
            [(ids_h, ids), (stream_h, stream), (gain_h, gain), (router_h, router), (w_up, up), (w_down, down)]
        )
    ]
    for c in loads:
        c.start()
    cu, cd = loads[4:]

    loads[0].wait()
    lane = lax.broadcasted_iota(jnp.int32, (tok, LANES), 1)
    row = lax.broadcasted_iota(jnp.int32, (LANES, tok), 0)
    ti = lax.broadcasted_iota(jnp.int32, (tok, tok), 0)
    tj = lax.broadcasted_iota(jnp.int32, (tok, tok), 1)
    before = (ti > tj).astype(F32).astype(BF)
    same = (ti == tj).astype(F32).astype(BF)
    for d in range(2):
        chosen = ids[d, 0]
        turned = jnp.zeros((LANES, tok), F32)
        for k in range(chosen.shape[0]):
            turned = turned + (chosen[k : k + 1] == row).astype(F32)
        turned = turned.astype(BF)
        hot = nt_dot(same, turned)
        earlier = nt_dot(before, turned)
        hots[d] = hot
        codes[d, c1[d]] = (hot * (earlier + 1.0)).astype(BF)
    loads[1].wait()
    pl.semaphore_wait(barrier, len(peers))

    for d in range(2):
        dev = {"pipe": lax.rem(p + (1 if d == 0 else np_ - 1), np_)}
        send(stream.at[d, 0], arr.at[d], shift_ss.at[d], shift_rs.at[d], dev)
    for d in range(2):
        for k in ahead(n1[d]):
            j = lax.rem(c1[d] + k, n1[d])
            here = codes.at[d, c1[d]]
            send(here, here, code_ss.at[d, k], code_rs.at[d, k], to_expert(at1(d, j)))
    loads[2].wait()
    loads[3].wait()
    for i, part in enumerate(split3(router[0] * gain[...])):
        rparts[i * experts : (i + 1) * experts] = part

    a = nx
    first = 1 - p % 2
    for d in (first, 1 - first):
        copy(stream.at[d, 0], arr.at[d], shift_ss.at[d], shift_rs.at[d], {"pipe": p}).wait_recv()
        own = coord1(d)
        for k in ahead(a):
            j = lax.rem(own + k, a)
            send(arr.at[d], blocks.at[d, own], block_ss.at[d, k], block_rs.at[d, k], to_expert(at1(d, j)))
        raw = arr[d]
        blocks[d, own] = raw
        wide = raw.astype(F32)
        squares = jnp.sum(wide * wide, axis=-1, keepdims=True)
        prod = nt_dot(raw, rparts[...])
        partial = prod[:, :experts] + (prod[:, experts : 2 * experts] + prod[:, 2 * experts : 3 * experts])
        stat_s[d, :, :experts] = partial
        stat_s[d, :, experts:] = jnp.broadcast_to(squares, (tok, LANES - experts))
        for k in range(1, nt):
            q = lax.rem(t + k, nt)
            send(stat_s.at[d], stat_r.at[d, k], stat_ss.at[d, k], stat_rs.at[d, k], {"tensor": q})
    for d in (first, 1 - first):
        total = stat_s[d]
        for k in range(1, nt):
            copy(stat_s.at[d], stat_r.at[d, k], stat_ss.at[d, k], stat_rs.at[d, k], {"tensor": t}).wait_recv()
            total = total + stat_r[d, k]
        inverse = lax.rsqrt(total[:, experts : experts + 1] / width + norm_eps)
        scores = jax.nn.sigmoid(total * inverse) * hots[d]
        gates = route_scale * scores / jnp.sum(scores, axis=-1, keepdims=True)
        own = coord1(d)
        info[d, own] = jnp.where(lane < experts, gates, jnp.broadcast_to(inverse, (tok, LANES)))
        for k in ahead(a):
            j = lax.rem(own + k, a)
            here = info.at[d, own]
            send(here, here, info_ss.at[d, k], info_rs.at[d, k], to_expert(at1(d, j)))

    b = nx
    nr, nc = a * b * cap, a * tok
    for d in (first, 1 - first):
        own = coord1(d)
        for k in range(1, a):
            j = lax.rem(own + a - k, a)
            copy(codes.at[d, j], codes.at[d, j], code_ss.at[d, k], code_rs.at[d, k], to_expert(e)).wait_recv()
        code = codes[d].reshape(nc, LANES)
        rr = lax.broadcasted_iota(jnp.int32, (nr, LANES), 0)
        at = at2(d, over(rr, per, nr))
        pick = (lax.broadcasted_iota(jnp.int32, (nr, LANES), 1) == at).astype(F32).astype(BF)

        def chosen_of(shape, rdim, value):
            r = lax.broadcasted_iota(jnp.int32, shape, rdim)
            c = lax.broadcasted_iota(jnp.int32, shape, 1 - rdim)
            third = over(r, cap, nr)
            slot = r - third * cap
            block = third - over(r, per, nr) * a
            return (value == (slot + 1).astype(F32)) & (block == over(c, tok, nc))

        sel = chosen_of((nr, nc), 0, nt_dot(pick, code)).astype(F32).astype(BF)
        keep = chosen_of((nc, nr), 1, nt_dot(code, pick))
        for k in range(1, a):
            j = lax.rem(own + a - k, a)
            copy(info.at[d, j], info.at[d, j], info_ss.at[d, k], info_rs.at[d, k], to_expert(e)).wait_recv()
        for k in range(1, a):
            j = lax.rem(own + a - k, a)
            copy(arr.at[d], blocks.at[d, j], block_ss.at[d, k], block_rs.at[d, k], to_expert(e)).wait_recv()
        facts = info[d].reshape(nc, LANES)
        inv = facts[:, experts : experts + 1]
        hidden = (blocks[d].reshape(nc, quarter).astype(F32) * gain[...] * inv).astype(BF)
        picked = mm(sel, hidden)
        for j in range(b):
            sel_s[d, j] = picked[j * per : (j + 1) * per].astype(BF)
        over2 = coord2(d)
        for g in range(3):
            for k in ahead(b):
                if k in parts[g]:
                    j = lax.rem(over2 + k, b)
                    to = rows.at[place[0, k] + d * len(parts[g])]
                    send(sel_s.at[d, j], to, sel_ss.at[d, k], sel_rs.at[d, k], to_expert(at2(d, j)))
        rows[place[0, 0] + d * len(parts[0])] = sel_s[d, over2]
        ghi = facts.astype(BF)
        glo = (facts - ghi.astype(F32)).astype(BF)
        mixers[d, 0] = jnp.where(keep, nt_dot(ghi, pick), 0.0).astype(BF)
        mixers[d, 1] = jnp.where(keep, nt_dot(glo, pick), 0.0).astype(BF)

    end = (t == 0) | (t == nt - 1)
    pair = t + 1 - 2 * (t % 2)
    flip, turn = nt - 1 - t, lax.rem(t + 2, nt)
    far_end = jnp.where(end, flip, turn)
    far_mid = jnp.where(end, turn, flip)

    def columns(q):
        return up[:, pl.ds(pl.multiple_of(q * fq, fq), fq)]

    side = (far_end, far_mid)

    def over_copy(g, i, q):
        o = over_s.at[i, spans[g]]
        return copy(o, over_r.at[i, spans[g]], over_ss.at[g, i], over_rs.at[g, i], {"tensor": q})

    def straight_copy(g, i, o, q):
        c = over_s.at[i, spans[g]]
        return copy(c, over_r.at[o, spans[g]], over_ss.at[g, i], over_rs.at[g, o], {"tensor": q})

    def pair_copy(g):
        return copy(pair_s.at[spans[g]], pair_r.at[spans[g]], pair_ss.at[g], pair_rs.at[g], {"tensor": pair})

    def cross_copy(g, i, q):
        return copy(over_s.at[i, spans[g]], cross_r.at[spans[g]], over_ss.at[g, i], cross_rs.at[g], {"tensor": q})

    def act_copy(g, q, i, o, to):
        c = act.at[q, spans[g]]
        return copy(c, c, act_ss.at[g, o], act_rs.at[g, i], {"tensor": to})

    def go(c):
        c.start()
        started.append(c)

    def at_end(f):
        pl.when(end)(f)

    def at_mid(f):
        pl.when(jnp.logical_not(end))(f)

    def arrive(g):
        for d in range(2):
            for k in parts[g]:
                if k:
                    copy(sel_s.at[d, 0], rows.at[place[d, k]], sel_ss.at[d, k], sel_rs.at[d, k], to_expert(e)).wait_recv()

    def upward(g):
        count = sizes[g]
        lhs = rows[firsts[g] : firsts[g] + count].reshape(count * per, quarter)
        for i in range(2):
            part = mm(lhs, columns(side[i]))
            if tree[g]:
                far_part[i, spans[g]] = part

                @at_end
                def _():
                    over_s[i, spans[g]] = far_part[i, spans[g]].astype(BF)
                    over_copy(g, i, pair).start()
            else:
                over_s[i, spans[g]] = part.astype(BF)
                at_end(lambda: straight_copy(g, i, 0, side[i]).start())
                at_mid(lambda: straight_copy(g, i, 1, side[i]).start())
        pair_s[spans[g]] = mm(lhs, columns(pair)).astype(BF)
        go(pair_copy(g))
        own_part[spans[g]] = mm(lhs, columns(t))

    def combine(g):
        if tree[g]:

            @at_mid
            def _():
                for i in range(2):
                    over_copy(g, i, t).wait_recv()
                    over_s[i, spans[g]] = (far_part[i, spans[g]] + over_r[i, spans[g]].astype(F32)).astype(BF)
                    cross_copy(g, i, side[i]).start()

    def activate(g):
        pair_copy(g).wait_recv()
        inner = own_part[spans[g]] + pair_r[spans[g]].astype(F32)
        if tree[g]:
            cross_copy(g, 0, t).wait_recv()
            inner = inner + cross_r[spans[g]].astype(F32)
        else:
            for o in range(2):
                straight_copy(g, 0, o, t).wait_recv()
                inner = inner + over_r[o, spans[g]].astype(F32)
        act[t, spans[g]] = jax.nn.silu(inner).astype(BF)

        @at_end
        def _():
            if not passed[g]:
                act_copy(g, t, 2, 2, far_end).start()
            act_copy(g, t, 2, 1, far_mid).start()

        @at_mid
        def _():
            if not passed[g]:
                act_copy(g, t, 1, 2, far_end).start()
            act_copy(g, t, 1, 1, far_mid).start()

        go(act_copy(g, t, 0, 0, pair))

    def relay(g):
        if passed[g]:

            @at_mid
            def _():
                act_copy(g, far_mid, 1, 2, t).wait_recv()
                act_copy(g, far_mid, 1, 2, pair).start()
                act_copy(g, far_end, 2, 3, t).wait_recv()
                act_copy(g, far_end, 2, 3, pair).start()

    def downward(g):
        def rest():
            act_copy(g, far_mid, 1, 2, t).wait_recv()
            act_copy(g, far_end, 2, 3, t).wait_recv()

        act_copy(g, pair, 0, 0, t).wait_recv()
        if passed[g]:
            at_end(rest)
        else:
            rest()
        lhs = jnp.concatenate([act[q, spans[g]] for q in range(nt)], axis=1)
        step = min(256, quarter)
        for s in range(0, quarter, step):
            made = mm(lhs, down[:, s : s + step])
            for j in range(sizes[g]):
                made_s[firsts[g] + j, :, s : s + step] = made[j * per : (j + 1) * per].astype(BF)
        for k in sorted(parts[g], key=lambda k: -min(k, n2[0] - k)):
            for d in range(2):
                here = made_s.at[place[d, k]]
                if k:
                    j = lax.rem(c2[d] + n2[d] - k, n2[d])
                    send(here, made_r.at[d, c2[d]], made_ss.at[d, k], made_rs.at[d, k], to_expert(at2(d, j)))
                else:
                    made_r[d, c2[d]] = made_s[place[d, k]]

    cu.wait()
    arrive(0)
    upward(0)
    combine(0)
    arrive(1)
    upward(1)
    activate(0)
    combine(1)
    arrive(2)
    upward(2)
    relay(0)
    activate(1)
    combine(2)
    cd.wait()
    downward(0)
    relay(1)
    activate(2)
    downward(1)
    relay(2)
    downward(2)
    for g in range(3):
        act_copy(g, t, 1, 1, far_mid).wait_send()
        over_copy(g, 0, pair).wait_send()
        over_copy(g, 1, pair).wait_send()
        if passed[g]:

            @at_mid
            def _():
                act_copy(g, far_mid, 1, 2, pair).wait_send()
                act_copy(g, far_end, 2, 3, pair).wait_send()
        else:
            act_copy(g, t, 1, 2, far_end).wait_send()

    for d in (first, 1 - first):
        own, mine = coord1(d), coord2(d)
        for k in range(1, b):
            j = lax.rem(mine + k, b)
            copy(made_s.at[0], made_r.at[d, j], made_ss.at[d, k], made_rs.at[d, k], to_expert(e)).wait_recv()
        back = made_r[d].reshape(nr, quarter)
        mixed = mm(mixers[d, 0], back) + mm(mixers[d, 1], back)
        for j in range(a):
            mix_s[d, j] = mixed[j * tok : (j + 1) * tok].astype(BF)
        for k in ahead(a):
            j = lax.rem(own + k, a)
            send(mix_s.at[d, j], mix_r.at[d, k], mix_ss.at[d, k], mix_rs.at[d, k], to_expert(at1(d, j)))
    for d in (first, 1 - first):
        total = mix_s[d, coord1(d)].astype(F32)
        for k in range(1, a):
            copy(mix_s.at[d, 0], mix_r.at[d, k], mix_ss.at[d, k], mix_rs.at[d, k], to_expert(e)).wait_recv()
            total = total + mix_r[d, k].astype(F32)
        out[d, 0] = (arr[d].astype(F32) + total).astype(BF)
    for c in started:
        c.wait_send()


def solution(mesh, nz=8, nx=8, cap=3):
    np_, nt = mesh.shape["pipe"], mesh.shape["tensor"]

    def shards(stream, ids, gain, router, w_up, w_down):
        tok, quarter = stream.shape[2:]
        experts, ff = router.shape[2], w_up.shape[2]
        cfg = (np_, nz, nx, nt, tok, cap, experts, float(quarter * nt))
        big, per = max(nz, nx), (nx * cap, nz * cap)
        assert nx == nz
        nr, fq = nx * nz * cap, ff // nt
        V, S = pltpu.VMEM, pltpu.SemaphoreType.DMA
        whole = pl.BlockSpec(memory_space=V)
        far = pl.BlockSpec(memory_space=pl.ANY)
        vmem = [
            V(stream.shape, BF), V((2, 1, ids.shape[3], tok), jnp.int32), V(gain.shape, F32), V((1, experts, quarter), F32),
            V((quarter, ff), BF), V((ff, quarter), BF), V((3 * experts, quarter), BF),
            V((2, tok, quarter), BF), V((2, big, tok, quarter), BF), V((2, big, tok, LANES), BF), V((2, big, tok, LANES), F32),
            V((2, tok, LANES), F32), V((2, nt, tok, LANES), F32), V((2, tok, LANES), F32), V((2, 2, big * tok, nr), BF),
            V((2, big, per[0], quarter), BF), V((2 * big, per[0], quarter), BF),
            V((2, 2 * nr, fq), F32), V((2 * nr, fq), F32),
            V((2, 2 * nr, fq), BF), V((2, 2 * nr, fq), BF), V((2 * nr, fq), BF), V((2 * nr, fq), BF), V((2 * nr, fq), BF),
            V((nt, 2 * nr, fq), BF),
            V((2 * big, per[0], quarter), BF), V((2, big, per[0], quarter), BF),
            V((2, big, tok, quarter), BF), V((2, big, tok, quarter), BF),
        ]
        sems = [S((6,)), S((2,)), S((2,))] + [S((2, big))] * 6 + [S((2, nt))] * 2 + [S((2, big))] * 2 + [S((3, 2))] * 2 + [S((3,))] * 3 + [S((3, 4))] * 2 + [S((2, big))] * 4
        return pl.pallas_call(
            functools.partial(layer, cfg),
            out_shape=pltpu.VMEM(stream.shape, BF),
            in_specs=[pl.BlockSpec(memory_space=pltpu.HBM)] * 6,
            out_specs=whole,
            scratch_shapes=vmem + sems,
            compiler_params=pltpu.CompilerParams(
                collective_id=0, has_side_effects=True, vmem_limit_bytes=56 * 1024 * 1024
            ),
        )(stream, jnp.swapaxes(ids, 2, 3), gain, jnp.swapaxes(router, 1, 2), w_up[0], w_down[0])

    return jax.shard_map(
        shards,
        mesh=mesh,
        in_specs=(
            P(None, "pipe", "expert", "tensor"),
            P(None, "pipe", "expert", None),
            P("pipe", "tensor"),
            P("pipe", "tensor", None),
            P("expert", "tensor", None),
            P("expert", None, "tensor"),
        ),
        out_specs=P(None, "pipe", "expert", "tensor"),
        check_vma=False,
    )
```
